32 devices in a mesh: dp: 4 (over x, core), fsdp: 8 (over z, y).
Axes of the slice: x: 2, y: 2, z: 4, core: 2. Of those that a mesh axis runs over, the one named last changes fastest.
Arguments:
- frames: bfloat16 [32768, 1024], P(('dp', 'fsdp')), may hold values from -6 to 6
- clip_lengths: int32 [128], P(('dp', 'fsdp')), may hold values from 0 to 1024, as said below
- timesteps: int32 [128], P(('dp', 'fsdp')), may hold values from 0 to 999
- cotangent: bfloat16 [32768, 1024], P(('dp', 'fsdp')), may hold values from -6 to 6
- adaptive_weight: bfloat16 [1024, 6144], P('fsdp', 'dp'), may hold values from -0.1875 to 0.1875
- project_weight: bfloat16 [1024, 3072], P('fsdp', 'dp'), may hold values from -0.1875 to 0.1875
- output_weight: bfloat16 [1024, 1024], P('fsdp', 'dp'), may hold values from -0.5 to 0.5
- upward_weight: bfloat16 [1024, 2048], P('fsdp', 'dp'), may hold values from -0.1875 to 0.1875
- downward_weight: bfloat16 [2048, 1024], P('fsdp', 'dp'), may hold values from -0.25 to 0.25
Outputs:
- block_out: bfloat16 [32768, 1024], P(('dp', 'fsdp'))
- frames_grad: float32 [32768, 1024], P(('dp', 'fsdp'))
- adaptive_grad: float32 [1024, 6144], P('fsdp', 'dp')
- project_grad: float32 [1024, 3072], P('fsdp', 'dp')
- output_grad: float32 [1024, 1024], P('fsdp', 'dp')
- upward_grad: float32 [1024, 2048], P('fsdp', 'dp')
- downward_grad: float32 [2048, 1024], P('fsdp', 'dp')
The draws below stay inside these ranges and needn't reach their ends.
Inputs may be any that keep to these rules, and one draw needn't show every extreme that they name: `clip_lengths`: the clips of one device take at most 1024 slots together; in every draw some device holds a single clip of 1024 frames.
All inputs are finite; a program needn't handle non-finite values.
Results may differ from the reference program's by a relative error of at most 0.01.
Values may be sent and summed in bfloat16 or wider, within the bound.
A program may use at most 384 MiB of HBM per device.

```python
import math
import jax
import jax.numpy as jnp
from jax import lax

D = 1024
HEADS = 16
HEAD_DIM = 64
FF = 2048
FRAMES_DEV = 1024
CLIPS_DEV = 4
FRAMES = 32768
CLIPS = 128


def draw_clip_lengths(key, part):
    device_count = CLIPS // CLIPS_DEV
    keys_all = jax.random.split(key, 5)
    powers = jax.random.randint(keys_all[0], (device_count, CLIPS_DEV), 0, 8)
    factors = jax.random.randint(keys_all[1], (device_count, CLIPS_DEV), 1, 5)
    shares = factors * jnp.left_shift(jnp.ones_like(powers), powers)
    used_frames = FRAMES_DEV - jax.random.randint(keys_all[2], (device_count, 1), 0, FRAMES_DEV // 2 + 1)
    lengths = used_frames * shares // jnp.sum(shares, axis=1, keepdims=True)
    chosen = jax.random.randint(keys_all[3], (), 0, device_count)
    single = jax.random.randint(keys_all[4], (), 0, CLIPS_DEV)
    full_row = jnp.where(jnp.arange(CLIPS_DEV) == single, FRAMES_DEV, 0)
    lengths = jnp.where((jnp.arange(device_count) == chosen)[:, None], full_row[None, :], lengths)
    return lengths.reshape(-1).astype(jnp.int32)


def touch_ends(entries, key, smallest, high):
    extent = entries.shape
    place = [jax.random.randint(jax.random.fold_in(key, axis), (), 0, extent[axis]) for axis in range(len(extent))]
    entries = entries.at[tuple(place)].set(smallest)
    longest = extent.index(max(extent))
    place[longest] = (place[longest] + 1) % extent[longest]
    return entries.at[tuple(place)].set(high)


def steps_of(stream_key, extent, cuts, least, top_value):
    gain = 1.0
    for dim, parts in cuts:
        draws = jax.random.uniform(jax.random.fold_in(jax.random.fold_in(stream_key, 6), dim), (parts,), jnp.float32, least / len(cuts), top_value / len(cuts))
        gain = gain * jnp.repeat(jnp.exp(draws), extent[dim] // parts).reshape((-1,) + (1,) * (len(extent) - 1 - dim))
    return gain


def noise(own_key, shape, scale, bound, cuts=(), held_as=jnp.bfloat16):
    values = scale * jax.random.normal(own_key, shape, jnp.float32)
    if cuts:
        values = values * steps_of(own_key, shape, cuts, -0.22, 0.18)
    return jnp.clip(values, -bound, bound).astype(held_as)


def setup_inputs(seed: int = 0) -> dict:
    key_list = jax.random.split(jax.random.key(seed), 10)
    return {
        "frames": noise(key_list[0], (FRAMES, D), 1.0, 6.0, ((0, 32),)),
        "clip_lengths": draw_clip_lengths(jax.random.fold_in(key_list[9], 71), 0),
        "timesteps": touch_ends(jax.random.randint(key_list[2], (CLIPS,), 0, 1000), jax.random.fold_in(key_list[2], 1), 0, 999).astype(jnp.int32),
        "cotangent": noise(key_list[3], (FRAMES, D), 1.0, 6.0, ((0, 32),)),
        "adaptive_weight": noise(key_list[4], (D, 6 * D), D ** -0.5, 0.1875, ((0, 8), (1, 4))),
        "project_weight": noise(key_list[5], (D, 3 * D), D ** -0.5, 0.1875, ((0, 8), (1, 4))),
        "output_weight": noise(key_list[6], (D, D), (D // 8) ** -0.5, 0.5, ((0, 8), (1, 4))),
        "upward_weight": noise(key_list[7], (D, FF), D ** -0.5, 0.1875, ((0, 8), (1, 4))),
        "downward_weight": noise(key_list[8], (FF, D), (FF // 4) ** -0.5, 0.25, ((0, 8), (1, 4))),
    }


EPSILON = 1e-06
HIGHEST = lax.Precision.HIGHEST

@jax.custom_vjp
def low(v):
    return lax.optimization_barrier(v.astype(jnp.bfloat16)).astype(jnp.float32)

@jax.custom_vjp
def low_back(v):
    return v

def low_keep(v):
    return (low(v), None)

def low_pass(kept, grad):
    return (grad,)

def back_keep(v):
    return (v, None)

def back_low(kept, grad):
    return (low(grad),)
low.defvjp(low_keep, low_pass)
low_back.defvjp(back_keep, back_low)

def dot_high(left, right):
    return jnp.dot(left, right, precision=HIGHEST, preferred_element_type=jnp.float32)

def layer_norm(values):
    center = values - lax.optimization_barrier(jnp.mean(values, axis=-1, keepdims=True))
    spread = lax.optimization_barrier(jnp.mean(center * center, axis=-1, keepdims=True))
    return center * lax.rsqrt(spread + EPSILON)

def clip_layout(lengths, frame_count):
    clip_count = lengths.shape[0]
    lengths = lengths.astype(jnp.int32)
    endings = jnp.cumsum(lengths, dtype=jnp.int32)
    beginnings = endings - lengths
    frame_index = jnp.arange(frame_count, dtype=jnp.int32)
    segment = lax.optimization_barrier(jnp.sum((frame_index[:, None] >= endings[None, :]).astype(jnp.int32), axis=1, dtype=jnp.int32))
    member = segment[:, None] == jnp.arange(clip_count, dtype=jnp.int32)[None, :]
    position = frame_index - lax.optimization_barrier(jnp.sum(jnp.where(member, beginnings[None, :], 0), axis=1, dtype=jnp.int32))
    onehot = member.astype(jnp.float32)
    validity = (segment < clip_count).astype(jnp.float32)[:, None]
    return (segment, onehot, validity, position)

def time_table(steps, model_width):
    halfway = model_width // 2
    rates = jnp.exp(-math.log(10000.0) * jnp.arange(halfway, dtype=jnp.float32) / (halfway - 1))
    angles = steps.astype(jnp.float32)[:, None] * rates[None, :]
    return jnp.concatenate([jnp.sin(angles), jnp.cos(angles)], axis=-1)

def rotary_table(position, head_width):
    halfway = head_width // 2
    rates = jnp.exp(-math.log(10000.0) * jnp.arange(halfway, dtype=jnp.float32) / halfway)
    angles = position.astype(jnp.float32)[:, None] * rates[None, :]
    cosine = jnp.cos(angles)
    sine_table = jnp.sin(angles)
    return (jnp.concatenate([cosine, cosine], axis=-1), jnp.concatenate([sine_table, sine_table], axis=-1))

def rotate(values, cosine, sine_table):
    halfway = values.shape[-1] // 2
    turned = jnp.concatenate([-values[..., halfway:], values[..., :halfway]], axis=-1)
    return values * cosine[:, None, :] + turned * sine_table[:, None, :]

def attend_reference(queries, keys, values, segment):
    frame_count = queries.shape[0]
    block_rows = min(512, frame_count)
    block_count = frame_count // block_rows
    scale = queries.shape[-1] ** (-0.5)

    def one_block(pieces):
        query_block, segment_block = pieces
        scores = low_back(jnp.einsum('qhd,khd->hqk', query_block, keys, precision=HIGHEST) * scale)
        allowed = segment_block[:, None] == segment[None, :]
        scores = jnp.where(allowed[None], scores, -1000000000.0)
        maximum = lax.optimization_barrier(jnp.max(scores, axis=-1, keepdims=True))
        exponent = jnp.exp(scores - maximum)
        probs = exponent / lax.optimization_barrier(jnp.sum(exponent, axis=-1, keepdims=True))
        return jnp.einsum('hqk,khd->qhd', low(probs), values, precision=HIGHEST)
    mixed = lax.map(jax.checkpoint(one_block), (queries.reshape(block_count, block_rows, HEADS, HEAD_DIM), segment.reshape(block_count, block_rows)))
    return mixed.reshape(frame_count, HEADS, HEAD_DIM)

def reference(frames, clip_lengths, timesteps, cotangent, adaptive_weight, project_weight, output_weight, upward_weight, downward_weight):
    frame_count = FRAMES_DEV
    device_count = frames.shape[0] // frame_count
    clip_count = clip_lengths.shape[0] // device_count
    matrices = (adaptive_weight.astype(jnp.float32), project_weight.astype(jnp.float32), output_weight.astype(jnp.float32), upward_weight.astype(jnp.float32), downward_weight.astype(jnp.float32))
    stacked = (frames.reshape(device_count, frame_count, D), cotangent.reshape(device_count, frame_count, D), clip_lengths.reshape(device_count, clip_count), timesteps.reshape(device_count, clip_count))
    head_shape = (frame_count, HEADS, HEAD_DIM)

    def one_device(sums, inputs):
        block_in, block_cot, lengths, steps = inputs
        segment, onehot, validity, position = clip_layout(lengths, frame_count)
        cosine, sine_table = rotary_table(position, HEAD_DIM)
        context = low(jax.nn.silu(time_table(steps, D)))

        def forward(adapt, project, output, upward, downward, inputs_f):
            modulation = low_back(dot_high(context, adapt))
            per_frame = dot_high(onehot, modulation)
            shift_one, scale_one, gate_one, shift_two, scale_two, gate_two = jnp.split(per_frame, 6, axis=1)
            normed_one = layer_norm(inputs_f)
            attn_in = low(normed_one * (1.0 + scale_one) + shift_one)
            projected = low_back(dot_high(attn_in, project))
            queries = low(rotate(projected[:, :D].reshape(head_shape), cosine, sine_table))
            keys = low(rotate(projected[:, D:2 * D].reshape(head_shape), cosine, sine_table))
            values = low(projected[:, 2 * D:].reshape(head_shape))
            mixed = attend_reference(queries, keys, values, segment)
            attn_out = low_back(low(mixed.reshape(frame_count, D)))
            branch = low_back(dot_high(attn_out, output))
            middle = inputs_f + validity * gate_one * branch
            normed_two = layer_norm(middle)
            ffn_in = low(normed_two * (1.0 + scale_two) + shift_two)
            upward_act = low_back(dot_high(ffn_in, upward))
            hidden = low(jax.nn.gelu(upward_act, approximate=True))
            downward_act = low_back(dot_high(hidden, downward))
            return middle + validity * gate_two * downward_act
        result, pullback = jax.vjp(forward, matrices[0], matrices[1], matrices[2], matrices[3], matrices[4], block_in.astype(jnp.float32))
        grads = pullback(block_cot.astype(jnp.float32))
        sums = (sums[0] + grads[0], sums[1] + grads[1], sums[2] + grads[2], sums[3] + grads[3], sums[4] + grads[4])
        return (sums, (result.astype(jnp.bfloat16), grads[5]))
    initial = (jnp.zeros(matrices[0].shape, jnp.float32), jnp.zeros(matrices[1].shape, jnp.float32), jnp.zeros(matrices[2].shape, jnp.float32), jnp.zeros(matrices[3].shape, jnp.float32), jnp.zeros(matrices[4].shape, jnp.float32))
    sums, (outputs, input_grads) = lax.scan(one_device, initial, stacked)
    return (outputs.reshape(-1, D), input_grads.reshape(-1, D), sums[0], sums[1], sums[2], sums[3], sums[4])
```

```python
import functools
import math

import jax
import jax.numpy as jnp
from jax import lax
from jax.experimental import pallas as pl
from jax.experimental.pallas import tpu as pltpu
from jax.sharding import PartitionSpec as P

HEAD_DIM = 64
LANES = 128
EPSILON = 1e-06
MASKED = -1000000000.0
VMEM_LIMIT = 60 * 1024 * 1024
BF16 = jnp.bfloat16
F32 = jnp.float32
AXES = ("dp", "fsdp")


def dot_nn(a, b):
    return lax.dot_general(a, b, (((1,), (0,)), ((), ())), preferred_element_type=F32)


def dot_nt(a, b):
    return lax.dot_general(a, b, (((1,), (1,)), ((), ())), preferred_element_type=F32)


def clip_rows(seg, mod_ref, part, width, clips):
    rows = jnp.zeros((seg.shape[0], width), F32)
    for c in range(clips):
        rows = jnp.where(seg == c, mod_ref[c : c + 1, part * width : (part + 1) * width], rows)
    return rows


def norm_parts(values):
    center = values - jnp.mean(values, axis=-1, keepdims=True)
    spread = jnp.mean(center * center, axis=-1, keepdims=True)
    scale = lax.rsqrt(spread + EPSILON)
    return center * scale, scale


def norm_back(grad, normed, scale):
    mean_g = jnp.mean(grad, axis=-1, keepdims=True)
    mean_gn = jnp.mean(grad * normed, axis=-1, keepdims=True)
    return (grad - mean_g - normed * mean_gn) * scale


def clip_sums(member, values):
    high = values.astype(BF16)
    low = (values - high.astype(F32)).astype(BF16)
    return dot_nn(member, high) + dot_nn(member, low)


def turn(values):
    lane = lax.broadcasted_iota(jnp.int32, values.shape, 1) % HEAD_DIM
    half = HEAD_DIM // 2
    return jnp.where(
        lane < half, pltpu.roll(values, LANES - half, 1), pltpu.roll(values, half, 1)
    )


def project_kernel(clips, frames_ref, seg_ref, mod_ref, weight_ref, cos_ref, sin_ref, attn_ref, out_ref):
    width = frames_ref.shape[1]

    @pl.when(pl.program_id(0) == 0)
    def _():
        step = 256
        for r in range(0, frames_ref.shape[0], step):
            normed, _ = norm_parts(frames_ref[r : r + step].astype(F32))
            seg = seg_ref[r : r + step]
            shift = clip_rows(seg, mod_ref, 0, width, clips)
            scale = clip_rows(seg, mod_ref, 1, width, clips)
            attn_ref[r : r + step] = (normed * (1.0 + scale) + shift).astype(BF16)

    result = dot_nn(attn_ref[...], weight_ref[0])
    for c in range(0, result.shape[1], LANES):
        piece = result[:, c : c + LANES]
        out_ref[:, c : c + LANES] = (piece * cos_ref[0] + turn(piece) * sin_ref[0]).astype(BF16)


def project_call(frames, seg_col, mod, weight, cosine, sine, clips):
    count, width = frames.shape
    blocks, _, columns = weight.shape
    tile = 256 if columns % 256 == 0 else 128
    per_block = columns // tile
    per_part = width // tile
    whole = lambda u: (0, 0)
    return pl.pallas_call(
        functools.partial(project_kernel, clips),
        grid=(blocks * per_block,),
        in_specs=[
            pl.BlockSpec((count, width), whole),
            pl.BlockSpec((count, 1), whole),
            pl.BlockSpec(mod.shape, whole),
            pl.BlockSpec((1, width, tile), lambda u: (u // per_block, 0, u % per_block)),
            pl.BlockSpec((1, count, LANES), lambda u: (u // per_part, 0, 0)),
            pl.BlockSpec((1, count, LANES), lambda u: (u // per_part, 0, 0)),
        ],
        out_specs=[
            pl.BlockSpec((count, width), whole),
            pl.BlockSpec((count, tile), lambda u: (0, u)),
        ],
        out_shape=[
            jax.ShapeDtypeStruct((count, width), BF16),
            jax.ShapeDtypeStruct((count, blocks * columns), BF16),
        ],
        compiler_params=pltpu.CompilerParams(vmem_limit_bytes=VMEM_LIMIT),
        cost_estimate=pl.CostEstimate(
            flops=2 * count * width * blocks * columns,
            bytes_accessed=2 * (2 * count * width + width * blocks * columns + count * blocks * columns),
            transcendentals=0,
        ),
        name="project",
    )(frames, seg_col, mod, weight, cosine, sine)


CHUNK = 256


def lane_head(values, h):
    lane = lax.broadcasted_iota(jnp.int32, (1, LANES), 1)
    keep = ((lane >= h * HEAD_DIM) & (lane < (h + 1) * HEAD_DIM)).astype(BF16)
    return values * keep


def transposed(values):
    return values.astype(F32).T.astype(BF16)


def attend_kernel(single_ref, q_ref, k_ref, v_ref, segr_ref, segc_ref, out_ref, lse_ref, mixed):
    keys = k_ref[...]
    values_t = transposed(v_ref[...])
    count = keys.shape[0]

    def run(masked):
        for h in range(LANES // HEAD_DIM):
            rows = slice(h * HEAD_DIM, (h + 1) * HEAD_DIM)
            for start in range(0, count, CHUNK):
                part = slice(start, start + CHUNK)
                scores = dot_nt(keys, lane_head(q_ref[part, :], h))
                if masked:
                    scores = jnp.where(segc_ref[...] == segr_ref[:, part], scores, MASKED)
                top = jnp.max(scores, axis=0, keepdims=True)
                weight = jnp.exp(scores - top)
                total = jnp.sum(weight, axis=0, keepdims=True)
                product = dot_nn(values_t[rows], weight.astype(BF16))
                mixed[rows, part] = product / total
                lse_ref[0, h : h + 1, part] = top + jnp.log(total)

    pl.when(single_ref[0] == 1)(functools.partial(run, False))
    pl.when(single_ref[0] != 1)(functools.partial(run, True))
    out_ref[...] = mixed[...].T.astype(BF16)


def attend_call(single, qkv, seg_row, seg_col):
    count = qkv.shape[0]
    width = qkv.shape[1] // 3
    pairs = width // LANES
    block = lambda t: pl.BlockSpec((count, LANES), lambda p, s: (0, t * pairs + p))
    return pl.pallas_call(
        attend_kernel,
        grid_spec=pltpu.PrefetchScalarGridSpec(
            num_scalar_prefetch=1,
            grid=(pairs,),
            in_specs=[
                block(0),
                block(1),
                block(2),
                pl.BlockSpec((1, count), lambda p, s: (0, 0)),
                pl.BlockSpec((count, 1), lambda p, s: (0, 0)),
            ],
            out_specs=[
                block(0),
                pl.BlockSpec((1, LANES // HEAD_DIM, count), lambda p, s: (p, 0, 0)),
            ],
            scratch_shapes=[pltpu.VMEM((LANES, count), F32)],
        ),
        out_shape=[
            jax.ShapeDtypeStruct((count, width), BF16),
            jax.ShapeDtypeStruct((pairs, LANES // HEAD_DIM, count), F32),
        ],
        compiler_params=pltpu.CompilerParams(vmem_limit_bytes=VMEM_LIMIT),
        cost_estimate=pl.CostEstimate(
            flops=16 * count * count * width, bytes_accessed=8 * count * width, transcendentals=16 * count * count
        ),
        name="attend",
    )(single, qkv, qkv, qkv, seg_row, seg_col)


def attend_back_kernel(
    single_ref, q_ref, k_ref, v_ref, grad_ref, out_ref, lse_ref, segr_ref, segc_ref, cos_ref, sin_ref,
    result_ref, grad_q, grad_k, grad_v,
):
    keys = k_ref[...]
    values = v_ref[...]
    keys_t = transposed(keys)
    count = keys.shape[0]
    inner_t = (grad_ref[...].astype(F32) * out_ref[...].astype(F32)).T
    heads = LANES // HEAD_DIM

    def run(masked):
        for h in range(heads):
            rows = slice(h * HEAD_DIM, (h + 1) * HEAD_DIM)
            inner = jnp.sum(inner_t[rows], axis=0, keepdims=True)
            for start in range(0, count, CHUNK):
                part = slice(start, start + CHUNK)
                query = lane_head(q_ref[part, :], h)
                grad = lane_head(grad_ref[part, :], h)
                scores = dot_nt(keys, query)
                if masked:
                    scores = jnp.where(segc_ref[...] == segr_ref[:, part], scores, MASKED)
                probs = jnp.exp(scores - lse_ref[0, h : h + 1, part])
                grad_probs = dot_nt(values, grad)
                add_v = dot_nn(probs.astype(BF16), grad)
                grad_scores = (probs * (grad_probs - inner[:, part])).astype(BF16)
                add_k = dot_nn(grad_scores, query)
                if h == 0 and start == 0:
                    grad_v[...] = add_v
                    grad_k[...] = add_k
                else:
                    grad_v[...] += add_v
                    grad_k[...] += add_k
                grad_q[rows, part] = dot_nn(keys_t[rows], grad_scores)

    pl.when(single_ref[0] == 1)(functools.partial(run, False))
    pl.when(single_ref[0] != 1)(functools.partial(run, True))

    def back(grad):
        return grad * cos_ref[...] + turn(grad * sin_ref[...])

    result_ref[0] = back(grad_q[...].T * (HEAD_DIM ** -0.5)).astype(BF16)
    result_ref[1] = back(grad_k[...]).astype(BF16)
    result_ref[2] = grad_v[...].astype(BF16)


def attend_back_call(single, qkv, grad_mixed, attn_out, lse, seg_row, seg_col, cosine, sine):
    count, width = attn_out.shape
    pairs = width // LANES
    heads = LANES // HEAD_DIM
    block = lambda t: pl.BlockSpec((count, LANES), lambda p, s: (0, t * pairs + p))
    fixed = lambda shape: pl.BlockSpec(shape, lambda p, s: (0, 0))
    return pl.pallas_call(
        attend_back_kernel,
        grid_spec=pltpu.PrefetchScalarGridSpec(
            num_scalar_prefetch=1,
            grid=(pairs,),
            in_specs=[
                block(0),
                block(1),
                block(2),
                block(0),
                block(0),
                pl.BlockSpec((1, heads, count), lambda p, s: (p, 0, 0)),
                fixed((1, count)),
                fixed((count, 1)),
                fixed((count, LANES)),
                fixed((count, LANES)),
            ],
            out_specs=pl.BlockSpec((3, count, LANES), lambda p, s: (0, 0, p)),
            scratch_shapes=[
                pltpu.VMEM((LANES, count), F32),
                pltpu.VMEM((count, LANES), F32),
                pltpu.VMEM((count, LANES), F32),
            ],
        ),
        out_shape=jax.ShapeDtypeStruct((3, count, width), BF16),
        compiler_params=pltpu.CompilerParams(vmem_limit_bytes=VMEM_LIMIT),
        cost_estimate=pl.CostEstimate(
            flops=40 * count * count * width, bytes_accessed=16 * count * width, transcendentals=16 * count * count
        ),
        name="attend_back",
    )(single, qkv, qkv, qkv, grad_mixed, attn_out, lse, seg_row, seg_col, cosine, sine)


def by_columns(left, weight_ref):
    return jnp.concatenate([dot_nn(left, weight_ref[b]) for b in range(weight_ref.shape[0])], axis=1)


def by_rows(left, weight_ref):
    columns = weight_ref.shape[2]
    total = None
    for b in range(weight_ref.shape[0]):
        term = dot_nt(left[:, b * columns : (b + 1) * columns], weight_ref[b])
        total = term if total is None else total + term
    return total


def middle_kernel(
    clips, frames_ref, cot_ref, attn_ref, seg_ref, member_ref, mod_ref, wo_ref, wu_ref, wd_ref,
    block_ref, ffn_ref, hidden_ref, down_ref, up_ref, gmid_ref, gbranch_ref, gmixed_ref, sums_ref,
):
    width = frames_ref.shape[1]
    seg = seg_ref[...]
    member = member_ref[...]
    cot = cot_ref[...].astype(F32)
    branch = by_columns(attn_ref[...], wo_ref)
    gate_one = clip_rows(seg, mod_ref, 2, width, clips)
    middle = frames_ref[...].astype(F32) + gate_one * branch
    normed, scale_n = norm_parts(middle)
    scale_two = 1.0 + clip_rows(seg, mod_ref, 4, width, clips)
    ffn_in = (normed * scale_two + clip_rows(seg, mod_ref, 3, width, clips)).astype(BF16)
    ffn_ref[...] = ffn_in
    upward = by_columns(ffn_in, wu_ref)
    root = math.sqrt(2.0 / math.pi)
    square = upward * upward
    wave = jnp.tanh(root * upward * (1.0 + 0.044715 * square))
    half = 0.5 * (1.0 + wave)
    hidden = (upward * half).astype(BF16)
    hidden_ref[...] = hidden
    slope = half + 0.5 * upward * (1.0 - wave * wave) * (root * (1.0 + 3.0 * 0.044715 * square))
    downward = by_columns(hidden, wd_ref)
    gate_two = clip_rows(seg, mod_ref, 5, width, clips)
    block_ref[...] = (middle + gate_two * downward).astype(BF16)
    grad_down = (gate_two * cot).astype(BF16)
    down_ref[...] = grad_down
    grad_up = (by_rows(grad_down, wd_ref) * slope).astype(BF16)
    up_ref[...] = grad_up
    grad_ffn = by_rows(grad_up, wu_ref)
    grad_middle = cot + norm_back(grad_ffn * scale_two, normed, scale_n)
    gmid_ref[...] = grad_middle
    grad_branch = (gate_one * grad_middle).astype(BF16)
    gbranch_ref[...] = grad_branch
    gmixed_ref[...] = by_rows(grad_branch, wo_ref).astype(BF16)

    @pl.when(pl.program_id(0) == 0)
    def _():
        sums_ref[...] = jnp.zeros_like(sums_ref)

    for i, values in enumerate(
        (branch * grad_middle, grad_ffn, grad_ffn * normed, downward * cot)
    ):
        sums_ref[:, i * width : (i + 1) * width] += clip_sums(member, values)


def middle_call(frames, cotangent, attn_out, seg_col, member, mod, wo, wu, wd, clips):
    count, width = frames.shape
    hidden = wd.shape[1]
    tile = 256
    rows = lambda w: pl.BlockSpec((tile, w), lambda i: (i, 0))
    fixed2 = lambda a: pl.BlockSpec(a.shape, lambda i: (0, 0))
    held = lambda a: pl.BlockSpec(a.shape, lambda i: (0, 0, 0), pipeline_mode=pl.Buffered(1))
    shape = lambda w, t: jax.ShapeDtypeStruct((count, w), t)
    return pl.pallas_call(
        functools.partial(middle_kernel, clips),
        grid=(count // tile,),
        in_specs=[
            rows(width),
            rows(width),
            rows(width),
            rows(1),
            pl.BlockSpec((member.shape[0], tile), lambda i: (0, i)),
            fixed2(mod),
            held(wo),
            held(wu),
            held(wd),
        ],
        out_specs=[
            rows(width),
            rows(width),
            rows(hidden),
            rows(width),
            rows(hidden),
            rows(width),
            rows(width),
            rows(width),
            pl.BlockSpec((member.shape[0], 4 * width), lambda i: (0, 0)),
        ],
        out_shape=[
            shape(width, BF16),
            shape(width, BF16),
            shape(hidden, BF16),
            shape(width, BF16),
            shape(hidden, BF16),
            shape(width, F32),
            shape(width, BF16),
            shape(width, BF16),
            jax.ShapeDtypeStruct((member.shape[0], 4 * width), F32),
        ],
        compiler_params=pltpu.CompilerParams(vmem_limit_bytes=VMEM_LIMIT),
        cost_estimate=pl.CostEstimate(
            flops=4 * count * width * (width + 2 * hidden),
            bytes_accessed=2 * width * (width + 2 * hidden) + 30 * count * width,
            transcendentals=count * hidden,
        ),
        name="middle",
    )(frames, cotangent, attn_out, seg_col, member, mod, wo, wu, wd)


def tail_kernel(clips, frames_ref, gmid_ref, gp_ref, seg_ref, member_ref, mod_ref, wp_ref, out_ref, sums_ref):
    width = frames_ref.shape[1]
    columns = wp_ref.shape[2]
    step = min(columns, 256) if columns % 256 == 0 else LANES
    grad = None
    for b in range(wp_ref.shape[0]):
        for c in range(0, columns, step):
            at = b * columns + c
            part, col = at // width, at % width
            term = dot_nt(gp_ref[part, :, col : col + step], wp_ref[b, :, c : c + step])
            grad = term if grad is None else grad + term
    normed, scale_n = norm_parts(frames_ref[...].astype(F32))
    scale_one = 1.0 + clip_rows(seg_ref[...], mod_ref, 1, width, clips)
    out_ref[...] = gmid_ref[...] + norm_back(grad * scale_one, normed, scale_n)

    @pl.when(pl.program_id(0) == 0)
    def _():
        sums_ref[...] = jnp.zeros_like(sums_ref)

    member = member_ref[...]
    for i, values in enumerate((grad, grad * normed)):
        sums_ref[:, i * width : (i + 1) * width] += clip_sums(member, values)


def tail_call(frames, grad_middle, grad_projected, seg_col, member, mod, wp, clips):
    count, width = frames.shape
    tile = 256
    rows = lambda w: pl.BlockSpec((tile, w), lambda i: (i, 0))
    return pl.pallas_call(
        functools.partial(tail_kernel, clips),
        grid=(count // tile,),
        in_specs=[
            rows(width),
            rows(width),
            pl.BlockSpec((3, tile, width), lambda i: (0, i, 0)),
            rows(1),
            pl.BlockSpec((member.shape[0], tile), lambda i: (0, i)),
            pl.BlockSpec(mod.shape, lambda i: (0, 0)),
            pl.BlockSpec(wp.shape, lambda i: (0, 0, 0), pipeline_mode=pl.Buffered(1)),
        ],
        out_specs=[rows(width), pl.BlockSpec((member.shape[0], 2 * width), lambda i: (0, 0))],
        out_shape=[
            jax.ShapeDtypeStruct((count, width), F32),
            jax.ShapeDtypeStruct((member.shape[0], 2 * width), F32),
        ],
        compiler_params=pltpu.CompilerParams(vmem_limit_bytes=VMEM_LIMIT),
        cost_estimate=pl.CostEstimate(
            flops=6 * count * width * width, bytes_accessed=6 * width * width + 16 * count * width, transcendentals=0
        ),
        name="tail",
    )(frames, grad_middle, grad_projected, seg_col, member, mod, wp)


def clip_layout(lengths, frame_count):
    clip_count = lengths.shape[0]
    endings = jnp.cumsum(lengths, dtype=jnp.int32)
    beginnings = endings - lengths
    frame_index = jnp.arange(frame_count, dtype=jnp.int32)
    segment = jnp.sum(
        (frame_index[:, None] >= endings[None, :]).astype(jnp.int32), axis=1, dtype=jnp.int32
    )
    member = segment[:, None] == jnp.arange(clip_count, dtype=jnp.int32)[None, :]
    position = frame_index - jnp.sum(
        jnp.where(member, beginnings[None, :], 0), axis=1, dtype=jnp.int32
    )
    return segment, position


def rotary_tables(position):
    half = HEAD_DIM // 2
    rates = jnp.exp(-math.log(10000.0) * jnp.arange(half, dtype=F32) / half)
    angles = position.astype(F32)[:, None] * rates[None, :]
    cosine, sine = jnp.cos(angles), jnp.sin(angles)
    copies = LANES // HEAD_DIM
    return (
        jnp.concatenate([cosine, cosine] * copies, axis=1),
        jnp.concatenate([-sine, sine] * copies, axis=1),
    )


def gather_blocks(weight, blocks):
    full = lax.all_gather(weight, AXES, axis=0, tiled=True)
    return full.reshape(blocks, full.shape[0] // blocks, full.shape[1])


def scatter_blocks(left, right, blocks):
    local = lax.dot_general(left, right, (((0,), (0,)), ((), ())), preferred_element_type=F32).astype(BF16)
    rows = local.shape[0]
    local = local.reshape(rows, blocks, -1).transpose(1, 0, 2).reshape(blocks * rows, -1)
    return lax.psum_scatter(local, AXES, scatter_dimension=0, tiled=True).astype(F32)


def per_device(
    blocks, row_parts, frames, clip_lengths, timesteps, cotangent,
    adaptive_weight, project_weight, output_weight, upward_weight, downward_weight,
):
    count, width = frames.shape
    clips = clip_lengths.shape[0]
    devices = blocks * row_parts
    segment, position = clip_layout(clip_lengths, count)
    seg_row, seg_col = segment[None, :], segment[:, None]
    single = (segment[0] == segment[count - 1]).astype(jnp.int32)[None]
    pad = -clips % 8
    member = (jnp.arange(clips + pad, dtype=jnp.int32)[:, None] == seg_row) & (seg_row < clips)
    member = member.astype(BF16)
    cosine, sine = rotary_tables(position)

    wp = gather_blocks(project_weight, blocks)
    steps = lax.all_to_all(
        jnp.broadcast_to(timesteps[None, :], (devices, clips)), AXES, 0, 0, tiled=True
    ).reshape(-1)
    rows, columns = adaptive_weight.shape
    half = width // 2
    index = lax.axis_index("fsdp") * rows + jnp.arange(rows, dtype=jnp.int32)
    rates = jnp.exp(-math.log(10000.0) * (index % half).astype(F32) / (half - 1))
    angles = steps.astype(F32)[:, None] * rates[None, :]
    table = jnp.where(index[None, :] < half, jnp.sin(angles), jnp.cos(angles))
    context = jax.nn.silu(table).astype(BF16)
    partial_mod = jnp.dot(context, adaptive_weight, preferred_element_type=F32)
    pieces = lax.all_to_all(partial_mod.reshape(devices, clips, columns), AXES, 0, 0, tiled=True)
    mod = jnp.sum(pieces.reshape(blocks, row_parts, clips, columns), axis=1)
    mod = mod.transpose(1, 0, 2).reshape(clips, blocks * columns)
    mod = jnp.pad(mod, ((0, pad), (0, 0)))

    wo = gather_blocks(output_weight, blocks)
    wu = gather_blocks(upward_weight, blocks)
    wd = gather_blocks(downward_weight, blocks)

    scale = HEAD_DIM ** -0.5
    one = jnp.ones_like(cosine)
    attn_in, qkv = project_call(
        frames, seg_col, mod, wp,
        jnp.stack([cosine * scale, cosine, one]),
        jnp.stack([sine * scale, sine, 0.0 * one]),
        clips,
    )
    attn_out, lse = attend_call(single, qkv, seg_row, seg_col)
    block_out, ffn_in, hidden, grad_down, grad_up, grad_middle, grad_branch, grad_mixed, sums_two = middle_call(
        frames, cotangent, attn_out, seg_col, member, mod, wo, wu, wd, clips
    )
    downward_grad = scatter_blocks(hidden, grad_down, blocks)
    upward_grad = scatter_blocks(ffn_in, grad_up, blocks)
    output_grad = scatter_blocks(attn_out, grad_branch, blocks)
    grad_projected = attend_back_call(
        single, qkv, grad_mixed, attn_out, lse, seg_row, seg_col, cosine, sine
    )
    flat = grad_projected.transpose(1, 0, 2).reshape(count, 3 * width)
    project_grad = scatter_blocks(attn_in, flat, blocks)
    frames_grad, sums_one = tail_call(
        frames, grad_middle, grad_projected, seg_col, member, mod, wp, clips
    )
    grad_mod = jnp.concatenate([sums_one, sums_two], axis=1)[:clips].astype(BF16)
    grad_mod = grad_mod.reshape(clips, blocks, columns).transpose(1, 0, 2)
    grad_mod = jnp.broadcast_to(grad_mod[:, None], (blocks, row_parts, clips, columns))
    grad_all = lax.all_to_all(grad_mod.reshape(devices, clips, columns), AXES, 0, 0, tiled=True)
    adaptive_grad = lax.dot_general(
        context, grad_all.reshape(devices * clips, columns), (((0,), (0,)), ((), ())), preferred_element_type=F32
    )
    return (block_out, frames_grad, adaptive_grad, project_grad, output_grad, upward_grad, downward_grad)


def solution(mesh):
    data = P(AXES, None)
    flat = P(AXES)
    weight = P("fsdp", "dp")
    return jax.shard_map(
        functools.partial(per_device, mesh.shape["dp"], mesh.shape["fsdp"]),
        mesh=mesh,
        in_specs=(data, flat, flat, data) + (weight,) * 5,
        out_specs=(data, data) + (weight,) * 5,
        check_vma=False,
    )
```

```python
import functools
import math

import jax
import jax.numpy as jnp
from jax import lax
from jax.experimental import pallas as pl
from jax.experimental.pallas import tpu as pltpu
from jax.sharding import PartitionSpec as P

HEAD_DIM = 64
LANES = 128
EPSILON = 1e-06
MASKED = -1000000000.0
VMEM_LIMIT = 60 * 1024 * 1024
BF16 = jnp.bfloat16
F32 = jnp.float32
AXES = ("dp", "fsdp")


def dot_nn(a, b):
    return lax.dot_general(a, b, (((1,), (0,)), ((), ())), preferred_element_type=F32)


def dot_nt(a, b):
    return lax.dot_general(a, b, (((1,), (1,)), ((), ())), preferred_element_type=F32)


def clip_rows(seg, mod_ref, part, width, clips):
    rows = jnp.zeros((seg.shape[0], width), F32)
    for c in range(clips):
        rows = jnp.where(seg == c, mod_ref[c : c + 1, part * width : (part + 1) * width], rows)
    return rows


def norm_parts(values):
    center = values - jnp.mean(values, axis=-1, keepdims=True)
    spread = jnp.mean(center * center, axis=-1, keepdims=True)
    scale = lax.rsqrt(spread + EPSILON)
    return center * scale, scale


def norm_back(grad, normed, scale):
    mean_g = jnp.mean(grad, axis=-1, keepdims=True)
    mean_gn = jnp.mean(grad * normed, axis=-1, keepdims=True)
    return (grad - mean_g - normed * mean_gn) * scale


def clip_sums(member, values):
    high = values.astype(BF16)
    low = (values - high.astype(F32)).astype(BF16)
    return dot_nn(member, high) + dot_nn(member, low)


def turn(values):
    lane = lax.broadcasted_iota(jnp.int32, values.shape, 1) % HEAD_DIM
    half = HEAD_DIM // 2
    return jnp.where(
        lane < half, pltpu.roll(values, LANES - half, 1), pltpu.roll(values, half, 1)
    )


def project_kernel(clips, frames_ref, seg_ref, mod_ref, weight_ref, cos_ref, sin_ref, turned_ref, out_ref, attn_ref):
    width = frames_ref.shape[1]

    @pl.when(pl.program_id(0) == 0)
    def _():
        step = 256
        for r in range(0, frames_ref.shape[0], step):
            normed, _ = norm_parts(frames_ref[r : r + step].astype(F32))
            seg = seg_ref[r : r + step]
            shift = clip_rows(seg, mod_ref, 0, width, clips)
            scale = clip_rows(seg, mod_ref, 1, width, clips)
            attn_in = (normed * (1.0 + scale) + shift).astype(BF16)
            attn_ref[r : r + step] = attn_in
            turned_ref[:, r : r + step] = attn_in.T

    result = dot_nn(attn_ref[...], weight_ref[0])
    for c in range(0, result.shape[1], LANES):
        piece = result[:, c : c + LANES]
        out_ref[:, c : c + LANES] = (piece * cos_ref[0] + turn(piece) * sin_ref[0]).astype(BF16)


def project_call(frames, seg_col, mod, weight, cosine, sine, clips):
    count, width = frames.shape
    blocks, _, columns = weight.shape
    tile = 256 if columns % 256 == 0 else 128
    per_block = columns // tile
    per_part = width // tile
    whole = lambda u: (0, 0)
    return pl.pallas_call(
        functools.partial(project_kernel, clips),
        grid=(blocks * per_block,),
        in_specs=[
            pl.BlockSpec((count, width), whole),
            pl.BlockSpec((count, 1), whole),
            pl.BlockSpec(mod.shape, whole),
            pl.BlockSpec((1, width, tile), lambda u: (u // per_block, 0, u % per_block)),
            pl.BlockSpec((1, count, LANES), lambda u: (u // per_part, 0, 0)),
            pl.BlockSpec((1, count, LANES), lambda u: (u // per_part, 0, 0)),
        ],
        out_specs=[
            pl.BlockSpec((width, count), whole),
            pl.BlockSpec((count, tile), lambda u: (0, u)),
        ],
        scratch_shapes=[pltpu.VMEM((count, width), BF16)],
        out_shape=[
            jax.ShapeDtypeStruct((width, count), BF16),
            jax.ShapeDtypeStruct((count, blocks * columns), BF16),
        ],
        compiler_params=pltpu.CompilerParams(vmem_limit_bytes=VMEM_LIMIT),
        cost_estimate=pl.CostEstimate(
            flops=2 * count * width * blocks * columns,
            bytes_accessed=2 * (2 * count * width + width * blocks * columns + count * blocks * columns),
            transcendentals=0,
        ),
        name="project",
    )(frames, seg_col, mod, weight, cosine, sine)


CHUNK = 256


def lane_head(values, h):
    lane = lax.broadcasted_iota(jnp.int32, (1, LANES), 1)
    keep = ((lane >= h * HEAD_DIM) & (lane < (h + 1) * HEAD_DIM)).astype(BF16)
    return values * keep


def transposed(values):
    return values.T


def attend_kernel(single_ref, q_ref, k_ref, v_ref, segr_ref, segc_ref, out_ref, turned_ref, lse_ref, mixed):
    keys = k_ref[...]
    values_t = transposed(v_ref[...])
    count = keys.shape[0]

    def run(masked):
        for h in range(LANES // HEAD_DIM):
            rows = slice(h * HEAD_DIM, (h + 1) * HEAD_DIM)
            for start in range(0, count, CHUNK):
                part = slice(start, start + CHUNK)
                scores = dot_nt(keys, lane_head(q_ref[part, :], h))
                if masked:
                    scores = jnp.where(segc_ref[...] == segr_ref[:, part], scores, MASKED)
                top = jnp.max(scores, axis=0, keepdims=True)
                weight = jnp.exp(scores - top)
                total = jnp.sum(weight, axis=0, keepdims=True)
                product = dot_nn(values_t[rows], weight.astype(BF16))
                mixed[rows, part] = product / total
                lse_ref[0, h : h + 1, part] = top + jnp.log(total)

    pl.when(single_ref[0] == 1)(functools.partial(run, False))
    pl.when(single_ref[0] != 1)(functools.partial(run, True))
    low = mixed[...].astype(BF16)
    turned_ref[...] = low
    out_ref[...] = low.T


def attend_call(single, qkv, seg_row, seg_col):
    count = qkv.shape[0]
    width = qkv.shape[1] // 3
    pairs = width // LANES
    block = lambda t: pl.BlockSpec((count, LANES), lambda p, s: (0, t * pairs + p))
    return pl.pallas_call(
        attend_kernel,
        grid_spec=pltpu.PrefetchScalarGridSpec(
            num_scalar_prefetch=1,
            grid=(pairs,),
            in_specs=[
                block(0),
                block(1),
                block(2),
                pl.BlockSpec((1, count), lambda p, s: (0, 0)),
                pl.BlockSpec((count, 1), lambda p, s: (0, 0)),
            ],
            out_specs=[
                block(0),
                pl.BlockSpec((LANES, count), lambda p, s: (p, 0)),
                pl.BlockSpec((1, LANES // HEAD_DIM, count), lambda p, s: (p, 0, 0)),
            ],
            scratch_shapes=[pltpu.VMEM((LANES, count), F32)],
        ),
        out_shape=[
            jax.ShapeDtypeStruct((count, width), BF16),
            jax.ShapeDtypeStruct((width, count), BF16),
            jax.ShapeDtypeStruct((pairs, LANES // HEAD_DIM, count), F32),
        ],
        compiler_params=pltpu.CompilerParams(vmem_limit_bytes=VMEM_LIMIT),
        cost_estimate=pl.CostEstimate(
            flops=16 * count * count * width, bytes_accessed=8 * count * width, transcendentals=16 * count * count
        ),
        name="attend",
    )(single, qkv, qkv, qkv, seg_row, seg_col)


def attend_back_kernel(
    single_ref, q_ref, k_ref, v_ref, grad_ref, out_ref, lse_ref, segr_ref, segc_ref, cos_ref, sin_ref,
    *rest,
):
    result_ref, grad_q, grad_k, grad_v = rest[-4:]
    keys = k_ref[...]
    values = v_ref[...]
    keys_t = transposed(keys)
    count = keys.shape[0]
    inner_t = (grad_ref[...].astype(F32) * out_ref[...].astype(F32)).T
    heads = LANES // HEAD_DIM

    def run(masked):
        for h in range(heads):
            rows = slice(h * HEAD_DIM, (h + 1) * HEAD_DIM)
            inner = jnp.sum(inner_t[rows], axis=0, keepdims=True)
            for start in range(0, count, CHUNK):
                part = slice(start, start + CHUNK)
                query = lane_head(q_ref[part, :], h)
                grad = lane_head(grad_ref[part, :], h)
                scores = dot_nt(keys, query)
                if masked:
                    scores = jnp.where(segc_ref[...] == segr_ref[:, part], scores, MASKED)
                probs = jnp.exp(scores - lse_ref[0, h : h + 1, part])
                grad_probs = dot_nt(values, grad)
                add_v = dot_nn(probs.astype(BF16), grad)
                grad_scores = (probs * (grad_probs - inner[:, part])).astype(BF16)
                add_k = dot_nn(grad_scores, query)
                if h == 0 and start == 0:
                    grad_v[...] = add_v
                    grad_k[...] = add_k
                else:
                    grad_v[...] += add_v
                    grad_k[...] += add_k
                grad_q[rows, part] = dot_nn(keys_t[rows], grad_scores)

    pl.when(single_ref[0] == 1)(functools.partial(run, False))
    pl.when(single_ref[0] != 1)(functools.partial(run, True))

    def back(grad):
        return grad * cos_ref[...] + turn(grad * sin_ref[...])

    result_ref[0] = back(grad_q[...].T * (HEAD_DIM ** -0.5)).astype(BF16)
    result_ref[1] = back(grad_k[...]).astype(BF16)
    result_ref[2] = grad_v[...].astype(BF16)


def attend_back_call(first, number, before, single, qkv, grad_mixed, attn_out, lse, seg_row, seg_col, cosine, sine):
    count, width = attn_out.shape
    pairs = width // LANES
    heads = LANES // HEAD_DIM
    block = lambda t: pl.BlockSpec((count, LANES), lambda p, s: (0, t * pairs + first + p))
    extra = [] if before is None else [before]
    fixed = lambda shape: pl.BlockSpec(shape, lambda p, s: (0, 0))
    return pl.pallas_call(
        attend_back_kernel,
        grid_spec=pltpu.PrefetchScalarGridSpec(
            num_scalar_prefetch=1,
            grid=(number,),
            in_specs=[
                block(0),
                block(1),
                block(2),
                block(0),
                block(0),
                pl.BlockSpec((1, heads, count), lambda p, s: (first + p, 0, 0)),
                fixed((1, count)),
                fixed((count, 1)),
                fixed((count, LANES)),
                fixed((count, LANES)),
            ] + [pl.BlockSpec(memory_space=pl.ANY)] * len(extra),
            out_specs=pl.BlockSpec((3, count, LANES), lambda p, s: (0, 0, first + p)),
            scratch_shapes=[
                pltpu.VMEM((LANES, count), F32),
                pltpu.VMEM((count, LANES), F32),
                pltpu.VMEM((count, LANES), F32),
            ],
        ),
        out_shape=jax.ShapeDtypeStruct((3, count, width), BF16),
        compiler_params=pltpu.CompilerParams(vmem_limit_bytes=VMEM_LIMIT),
        cost_estimate=pl.CostEstimate(
            flops=40 * count * count * LANES * number,
            bytes_accessed=16 * count * LANES * number,
            transcendentals=2 * count * count * number,
        ),
        input_output_aliases={11: 0} if extra else {},
        name="attend_back",
    )(single, qkv, qkv, qkv, grad_mixed, attn_out, lse, seg_row, seg_col, cosine, sine, *extra)


def by_columns(left, pieces):
    return jnp.concatenate([dot_nn(left, piece) for piece in pieces], axis=1)


def by_rows(left, pieces):
    columns = pieces[0].shape[1]
    total = None
    for b, piece in enumerate(pieces):
        term = dot_nt(left[:, b * columns : (b + 1) * columns], piece)
        total = term if total is None else total + term
    return total


def middle_kernel(
    clips, frames_ref, cot_ref, attn_ref, seg_ref, member_ref, mod_ref, weights_ref,
    block_ref, ffn_ref, hidden_ref, down_ref, up_ref, gmid_ref, gbranch_ref, gmixed_ref, sums_ref,
):
    width = frames_ref.shape[1]
    seg = seg_ref[...]
    member = member_ref[...]
    cot = cot_ref[...].astype(F32)
    blocks, parts, height, columns = weights_ref.shape
    unit = height // 5

    def piece(b, start, stop):
        rows = weights_ref[b, :, start * unit : stop * unit, :]
        return rows.reshape(parts * (stop - start) * unit, columns)

    wo = [piece(b, 0, 1) for b in range(blocks)]
    wu = [piece(b, 1 + j, 2 + j) for b in range(blocks) for j in range(2)]
    wd = [piece(b, 3, 5) for b in range(blocks)]
    branch = by_columns(attn_ref[...], wo)
    gate_one = clip_rows(seg, mod_ref, 2, width, clips)
    middle = frames_ref[...].astype(F32) + gate_one * branch
    normed, scale_n = norm_parts(middle)
    scale_two = 1.0 + clip_rows(seg, mod_ref, 4, width, clips)
    ffn_in = (normed * scale_two + clip_rows(seg, mod_ref, 3, width, clips)).astype(BF16)
    ffn_ref[...] = ffn_in.T
    upward = by_columns(ffn_in, wu)
    root = math.sqrt(2.0 / math.pi)
    square = upward * upward
    wave = jnp.tanh(root * upward * (1.0 + 0.044715 * square))
    half = 0.5 * (1.0 + wave)
    hidden = (upward * half).astype(BF16)
    hidden_ref[...] = hidden.T
    slope = half + 0.5 * upward * (1.0 - wave * wave) * (root * (1.0 + 3.0 * 0.044715 * square))
    downward = by_columns(hidden, wd)
    gate_two = clip_rows(seg, mod_ref, 5, width, clips)
    block_ref[...] = (middle + gate_two * downward).astype(BF16)
    grad_down = (gate_two * cot).astype(BF16)
    down_ref[...] = grad_down
    grad_up = (by_rows(grad_down, wd) * slope).astype(BF16)
    up_ref[...] = grad_up
    grad_ffn = by_rows(grad_up, wu)
    grad_middle = cot + norm_back(grad_ffn * scale_two, normed, scale_n)
    gmid_ref[...] = grad_middle
    grad_branch = (gate_one * grad_middle).astype(BF16)
    gbranch_ref[...] = grad_branch
    gmixed_ref[...] = by_rows(grad_branch, wo).astype(BF16)

    @pl.when(pl.program_id(0) == 0)
    def _():
        sums_ref[...] = jnp.zeros_like(sums_ref)

    for i, values in enumerate(
        (branch * grad_middle, grad_ffn, grad_ffn * normed, downward * cot)
    ):
        sums_ref[:, i * width : (i + 1) * width] += clip_sums(member, values)


def middle_call(frames, cotangent, attn_out, seg_col, member, mod, weights, clips):
    count, width = frames.shape
    hidden = 2 * width
    tile = 256
    rows = lambda w: pl.BlockSpec((tile, w), lambda i: (i, 0))
    fixed2 = lambda a: pl.BlockSpec(a.shape, lambda i: (0, 0))
    turned = lambda h: pl.BlockSpec((h, tile), lambda i: (0, i))
    shape = lambda w, t: jax.ShapeDtypeStruct((count, w), t)
    return pl.pallas_call(
        functools.partial(middle_kernel, clips),
        grid=(count // tile,),
        in_specs=[
            rows(width),
            rows(width),
            rows(width),
            rows(1),
            pl.BlockSpec((member.shape[0], tile), lambda i: (0, i)),
            fixed2(mod),
            pl.BlockSpec(weights.shape, lambda i: (0, 0, 0, 0), pipeline_mode=pl.Buffered(1)),
        ],
        out_specs=[
            rows(width),
            turned(width),
            turned(hidden),
            rows(width),
            rows(hidden),
            rows(width),
            rows(width),
            rows(width),
            pl.BlockSpec((member.shape[0], 4 * width), lambda i: (0, 0)),
        ],
        out_shape=[
            shape(width, BF16),
            jax.ShapeDtypeStruct((width, count), BF16),
            jax.ShapeDtypeStruct((hidden, count), BF16),
            shape(width, BF16),
            shape(hidden, BF16),
            shape(width, F32),
            shape(width, BF16),
            shape(width, BF16),
            jax.ShapeDtypeStruct((member.shape[0], 4 * width), F32),
        ],
        compiler_params=pltpu.CompilerParams(vmem_limit_bytes=VMEM_LIMIT),
        cost_estimate=pl.CostEstimate(
            flops=4 * count * width * (width + 2 * hidden),
            bytes_accessed=2 * width * (width + 2 * hidden) + 30 * count * width,
            transcendentals=count * hidden,
        ),
        name="middle",
    )(frames, cotangent, attn_out, seg_col, member, mod, weights)


def tail_kernel(clips, frames_ref, gmid_ref, gp_ref, seg_ref, member_ref, mod_ref, wp_ref, out_ref, sums_ref):
    width = frames_ref.shape[1]
    columns = wp_ref.shape[2]
    step = min(columns, 256) if columns % 256 == 0 else LANES
    grad = None
    for b in range(wp_ref.shape[0]):
        for c in range(0, columns, step):
            at = b * columns + c
            part, col = at // width, at % width
            term = dot_nt(gp_ref[part, :, col : col + step], wp_ref[b, :, c : c + step])
            grad = term if grad is None else grad + term
    normed, scale_n = norm_parts(frames_ref[...].astype(F32))
    scale_one = 1.0 + clip_rows(seg_ref[...], mod_ref, 1, width, clips)
    out_ref[...] = gmid_ref[...] + norm_back(grad * scale_one, normed, scale_n)

    @pl.when(pl.program_id(0) == 0)
    def _():
        sums_ref[...] = jnp.zeros_like(sums_ref)

    member = member_ref[...]
    for i, values in enumerate((grad, grad * normed)):
        sums_ref[:, i * width : (i + 1) * width] += clip_sums(member, values)


def tail_call(frames, grad_middle, grad_projected, seg_col, member, mod, wp, clips):
    count, width = frames.shape
    tile = 256
    rows = lambda w: pl.BlockSpec((tile, w), lambda i: (i, 0))
    return pl.pallas_call(
        functools.partial(tail_kernel, clips),
        grid=(count // tile,),
        in_specs=[
            rows(width),
            rows(width),
            pl.BlockSpec((3, tile, width), lambda i: (0, i, 0)),
            rows(1),
            pl.BlockSpec((member.shape[0], tile), lambda i: (0, i)),
            pl.BlockSpec(mod.shape, lambda i: (0, 0)),
            pl.BlockSpec(wp.shape, lambda i: (0, 0, 0), pipeline_mode=pl.Buffered(1)),
        ],
        out_specs=[rows(width), pl.BlockSpec((member.shape[0], 2 * width), lambda i: (0, 0))],
        out_shape=[
            jax.ShapeDtypeStruct((count, width), F32),
            jax.ShapeDtypeStruct((member.shape[0], 2 * width), F32),
        ],
        compiler_params=pltpu.CompilerParams(vmem_limit_bytes=VMEM_LIMIT),
        cost_estimate=pl.CostEstimate(
            flops=6 * count * width * width, bytes_accessed=6 * width * width + 16 * count * width, transcendentals=0
        ),
        name="tail",
    )(frames, grad_middle, grad_projected, seg_col, member, mod, wp)


def clip_layout(lengths, frame_count):
    clip_count = lengths.shape[0]
    endings = jnp.cumsum(lengths, dtype=jnp.int32)
    beginnings = endings - lengths
    frame_index = jnp.arange(frame_count, dtype=jnp.int32)
    segment = jnp.sum(
        (frame_index[:, None] >= endings[None, :]).astype(jnp.int32), axis=1, dtype=jnp.int32
    )
    member = segment[:, None] == jnp.arange(clip_count, dtype=jnp.int32)[None, :]
    position = frame_index - jnp.sum(
        jnp.where(member, beginnings[None, :], 0), axis=1, dtype=jnp.int32
    )
    return segment, position


def rotary_tables(position):
    half = HEAD_DIM // 2
    rates = jnp.exp(-math.log(10000.0) * jnp.arange(half, dtype=F32) / half)
    angles = position.astype(F32)[:, None] * rates[None, :]
    cosine, sine = jnp.cos(angles), jnp.sin(angles)
    copies = LANES // HEAD_DIM
    return (
        jnp.concatenate([cosine, cosine] * copies, axis=1),
        jnp.concatenate([-sine, sine] * copies, axis=1),
    )


def gather_blocks(weight, blocks):
    full = lax.all_gather(weight, AXES, axis=0, tiled=True)
    return full.reshape(blocks, full.shape[0] // blocks, full.shape[1])


def unit_kernel(order_ref, left_ref, right_ref, out_ref):
    out_ref[0] = dot_nn(left_ref[...], right_ref[0]).astype(BF16)


def unit_products(order, left, right, tile):
    rows, count = left.shape
    number = order.shape[0]
    per_part = right.shape[2] // tile
    return pl.pallas_call(
        unit_kernel,
        grid_spec=pltpu.PrefetchScalarGridSpec(
            num_scalar_prefetch=1,
            grid=(number,),
            in_specs=[
                pl.BlockSpec((rows, count), lambda i, o: (0, 0)),
                pl.BlockSpec((1, count, tile), lambda i, o: (o[i] // per_part, 0, o[i] % per_part)),
            ],
            out_specs=pl.BlockSpec((1, rows, tile), lambda i, o: (i, 0, 0)),
        ),
        out_shape=jax.ShapeDtypeStruct((number, rows, tile), BF16),
        compiler_params=pltpu.CompilerParams(vmem_limit_bytes=VMEM_LIMIT),
        cost_estimate=pl.CostEstimate(
            flops=2 * number * rows * count * tile,
            bytes_accessed=2 * (rows * count + number * tile * (rows + count)),
            transcendentals=0,
        ),
        name="unit_products",
    )(order, left, right)


def pair_kernel(attn_ref, ffn_ref, branch_ref, up_ref, out_ref):
    parts, height, tile = out_ref.shape[1:]

    @pl.when(pl.program_id(1) == 0)
    def _():
        out_ref[0] = dot_nn(attn_ref[...], branch_ref[...]).astype(BF16).reshape(parts, height, tile)

    @pl.when(pl.program_id(1) != 0)
    def _():
        out_ref[0] = dot_nn(ffn_ref[...], up_ref[...]).astype(BF16).reshape(parts, height, tile)


def pair_products(blocks, parts, tile, attn_t, ffn_t, grad_branch, grad_up):
    width, count = attn_t.shape
    height = width // parts
    fixed = pl.BlockSpec((width, count), lambda b, k: (0, 0))
    return pl.pallas_call(
        pair_kernel,
        grid=(blocks, 3),
        in_specs=[
            fixed,
            fixed,
            pl.BlockSpec((count, tile), lambda b, k: (0, b)),
            pl.BlockSpec((count, tile), lambda b, k: (0, 2 * b + jnp.maximum(k - 1, 0))),
        ],
        out_specs=pl.BlockSpec((1, parts, height, tile), lambda b, k: (b, 0, k, 0)),
        out_shape=jax.ShapeDtypeStruct((blocks, parts, 3 * height, tile), BF16),
        compiler_params=pltpu.CompilerParams(vmem_limit_bytes=VMEM_LIMIT),
        cost_estimate=pl.CostEstimate(
            flops=6 * blocks * tile * width * count, bytes_accessed=16 * count * width, transcendentals=0
        ),
        name="pair_products",
    )(attn_t, ffn_t, grad_branch, grad_up)


def halve(send, keep, stages, sizes):
    live = [("dp", b) for b in range(1, sizes["dp"].bit_length() - 1)]
    live += [("fsdp", b) for b in reversed(range(sizes["fsdp"].bit_length() - 1))]

    def exchange(values, axis, bit):
        return lax.ppermute(values, axis, [(i, i ^ (1 << bit)) for i in range(sizes[axis])])

    got = exchange(send, "dp", 0)
    for axis, bit in stages:
        at = live.index((axis, bit))
        live.pop(at)
        mine = 1 if axis == "dp" else (lax.axis_index(axis) >> bit) & 1

        def side(which):
            pick = lambda v: lax.dynamic_index_in_dim(v, which, at, keepdims=False).astype(F32)
            return pick(keep) + pick(got)

        send, keep = side(1 - mine).astype(BF16), side(mine)
        got = exchange(send, axis, bit)
    return keep.astype(F32) + got.astype(F32)


def stage_orders(sizes):
    dp = [("dp", b) for b in range(1, sizes["dp"].bit_length() - 1)]
    fsdp = [("fsdp", b) for b in range(sizes["fsdp"].bit_length() - 1)]
    return (dp + fsdp, fsdp[:1] + dp + fsdp[1:], fsdp[1:] + dp + fsdp[:1])


def near_order(blocks, lowest):
    bits = blocks.bit_length() - 1
    flips = []
    for place in range(blocks // 2):
        flip = 1 - lowest
        for b in range(1, bits):
            flip |= (1 - ((place >> (bits - 1 - b)) & 1)) << b
        flips.append(flip)
    return lax.axis_index("dp") ^ jnp.array(flips, jnp.int32)


def per_device(
    blocks, row_parts, frames, clip_lengths, timesteps, cotangent,
    adaptive_weight, project_weight, output_weight, upward_weight, downward_weight,
):
    count, width = frames.shape
    clips = clip_lengths.shape[0]
    devices = blocks * row_parts
    segment, position = clip_layout(clip_lengths, count)
    seg_row, seg_col = segment[None, :], segment[:, None]
    single = (segment[0] == segment[count - 1]).astype(jnp.int32)[None]
    pad = -clips % 8
    member = (jnp.arange(clips + pad, dtype=jnp.int32)[:, None] == seg_row) & (seg_row < clips)
    member = member.astype(BF16)
    cosine, sine = rotary_tables(position)

    wp = gather_blocks(project_weight, blocks)
    steps = lax.all_to_all(
        jnp.broadcast_to(timesteps[None, :], (devices, clips)), AXES, 0, 0, tiled=True
    ).reshape(-1)
    rows, columns = adaptive_weight.shape
    half = width // 2
    index = lax.axis_index("fsdp") * rows + jnp.arange(rows, dtype=jnp.int32)
    rates = jnp.exp(-math.log(10000.0) * (index % half).astype(F32) / (half - 1))
    angles = steps.astype(F32)[:, None] * rates[None, :]
    table = jnp.where(index[None, :] < half, jnp.sin(angles), jnp.cos(angles))
    context = jax.nn.silu(table).astype(BF16)
    partial_mod = jnp.dot(context, adaptive_weight, preferred_element_type=F32)
    pieces = lax.all_to_all(partial_mod.reshape(devices, clips, columns), AXES, 0, 0, tiled=True)
    mod = jnp.sum(pieces.reshape(blocks, row_parts, clips, columns), axis=1)
    mod = mod.transpose(1, 0, 2).reshape(clips, blocks * columns)
    mod = jnp.pad(mod, ((0, pad), (0, 0)))

    tile = output_weight.shape[1]
    shard = jnp.concatenate(
        [output_weight, upward_weight[:, :tile], upward_weight[:, tile:], downward_weight], axis=0
    )
    weights = lax.all_gather(shard, AXES, axis=0, tiled=True).reshape(blocks, row_parts, shard.shape[0], tile)

    scale = HEAD_DIM ** -0.5
    one = jnp.ones_like(cosine)
    attn_in_t, qkv = project_call(
        frames, seg_col, mod, wp,
        jnp.stack([cosine * scale, cosine, one]),
        jnp.stack([sine * scale, sine, 0.0 * one]),
        clips,
    )
    attn_out, attn_t, lse = attend_call(single, qkv, seg_row, seg_col)
    block_out, ffn_t, hidden_t, grad_down, grad_up, grad_middle, grad_branch, grad_mixed, sums_two = middle_call(
        frames, cotangent, attn_out, seg_col, member, mod, weights, clips
    )

    sizes = {"dp": blocks, "fsdp": row_parts}
    orders = stage_orders(sizes)
    bits = (2,) * (blocks.bit_length() - 2 + row_parts.bit_length() - 1)
    far, near = near_order(blocks, 0), near_order(blocks, 1)

    down_send = unit_products(far, hidden_t, grad_down[None], tile)
    down_keep = unit_products(near, hidden_t, grad_down[None], tile)
    shape = bits + downward_weight.shape
    downward_grad = halve(down_send.reshape(shape), down_keep.reshape(shape), orders[1], sizes)

    pair = pair_products(blocks, row_parts, tile, attn_t, ffn_t, grad_branch, grad_up)
    pair = lax.psum_scatter(pair.reshape(-1, tile), AXES, scatter_dimension=0, tiled=True).astype(F32)
    output_grad, upward_left, upward_right = jnp.split(pair, 3, axis=0)
    upward_grad = jnp.concatenate([upward_left, upward_right], axis=1)

    grad_projected = None
    number = width // LANES // 2
    for first in (0, number):
        grad_projected = attend_back_call(
            first, number, grad_projected,
            single, qkv, grad_mixed, attn_out, lse, seg_row, seg_col, cosine, sine,
        )
    units = project_weight.shape[1] // tile
    shape = bits + (project_weight.shape[0], tile)
    sends = [unit_products(far * units + j, attn_in_t, grad_projected, tile) for j in range(units)]
    keeps = unit_products(
        jnp.concatenate([near * units + j for j in range(units)]), attn_in_t, grad_projected, tile
    ).reshape((units,) + shape)
    project_grad = jnp.concatenate(
        [halve(sends[j].reshape(shape), keeps[j], orders[j % 3], sizes) for j in range(units)], axis=1
    )
    frames_grad, sums_one = tail_call(
        frames, grad_middle, grad_projected, seg_col, member, mod, wp, clips
    )
    grad_mod = jnp.concatenate([sums_one, sums_two], axis=1)[:clips].astype(BF16)
    grad_mod = grad_mod.reshape(clips, blocks, columns).transpose(1, 0, 2)
    grad_mod = jnp.broadcast_to(grad_mod[:, None], (blocks, row_parts, clips, columns))
    grad_all = lax.all_to_all(grad_mod.reshape(devices, clips, columns), AXES, 0, 0, tiled=True)
    adaptive_grad = lax.dot_general(
        context, grad_all.reshape(devices * clips, columns), (((0,), (0,)), ((), ())), preferred_element_type=F32
    )
    return (block_out, frames_grad, adaptive_grad, project_grad, output_grad, upward_grad, downward_grad)


def solution(mesh):
    data = P(AXES, None)
    flat = P(AXES)
    weight = P("fsdp", "dp")
    return jax.shard_map(
        functools.partial(per_device, mesh.shape["dp"], mesh.shape["fsdp"]),
        mesh=mesh,
        in_specs=(data, flat, flat, data) + (weight,) * 5,
        out_specs=(data, data) + (weight,) * 5,
        check_vma=False,
    )
```
